32 devices in a mesh: seq: 4 (over y, core), exp: 8 (over z, x).
Axes of the slice: x: 2, y: 2, z: 4, core: 2. Of those that a mesh axis runs over, the one named last changes fastest.
Arguments:
- residual_stream: bfloat16 [2048, 4096], P(('seq', 'exp')), may hold values from -6 to 6
- norm_gain: float32 [4096], replicated, may hold values from 0.25 to 1.75
- expert_ids: int32 [2048, 2], P(('seq', 'exp')), may hold values from 0 to 7, all different within a row; in each aligned block of 64 rows (0 to 63, 64 to 127, ...) at most 18 rows name the same one
- gate_weights: float32 [2048, 2], P(('seq', 'exp')), may hold values from 0.2 to 1
- w_gate: bfloat16 [8, 4096, 7168], P('exp', None, 'seq'), may hold values from -0.09375 to 0.09375
- w_up: bfloat16 [8, 4096, 7168], P('exp', None, 'seq'), may hold values from -0.09375 to 0.09375
- w_down: bfloat16 [8, 7168, 4096], P('exp', 'seq'), may hold values from -0.0625 to 0.0625
Outputs:
- moe_out: bfloat16 [2048, 4096], P(('seq', 'exp'))
The draws below stay inside these ranges and needn't reach their ends.
Inputs may be any that keep to these rules, and one draw needn't show every extreme that they name: `expert_ids`: each row names 2 different experts. In each aligned block of 64 rows (the rows of one device) no expert is named by more than 18 rows, a bound that some blocks reach.
All inputs are finite; a program needn't handle non-finite values.
Results may differ from the reference program's by a relative error of at most 0.015.
Values may be sent and summed in bfloat16 or wider, within the bound.
No kernel may reach another device: no remote copies, remote signals or barrier semaphores. Data moves between devices by JAX's collectives and lax.ppermute only.
A program may use at most 128 MiB of HBM per device.

```python
import math
import jax
import jax.numpy as jnp
import numpy as np
from jax import lax

D = 4096
FF = 7168
TOP = 2
TOK_DEV = 64
EXPERTS = 8
TOKENS = 2048
CAP = 18
N_SEQ = 4


def block_scale(own_key, extent, split, smallest, high):
    def one(dim, blocks):
        steps = jax.random.uniform(jax.random.fold_in(jax.random.fold_in(own_key, 6), dim), (blocks,), jnp.float32, smallest / len(split), high / len(split))
        return jnp.repeat(jnp.exp(steps), extent[dim] // blocks).reshape((-1,) + (1,) * (len(extent) - dim - 1))

    gain = one(*split[0])
    for cut in split[1:]:
        gain = gain * one(*cut)
    return gain


def deal_out(own_key, own, number, rows, count, top, reach, skew):
    ranking = jax.random.permutation(own_key, count)
    packed, ordinary = load_shares(count, rows * top, reach, skew, True), load_shares(count, rows * top, reach, skew, False)
    places = jnp.arange(count)

    def named(tallies, turn):
        used = int((tallies > 0).sum())
        fixed = max(1, used // 4)
        passed = fixed + (places - fixed + turn * (used - fixed)) % max(1, count - fixed)
        return jnp.zeros((count,), jnp.int32).at[ranking[jnp.where(places < fixed, places, passed)]].set(jnp.asarray(tallies, jnp.int32))

    tallies = jnp.where(number % 4 == 0, named(packed, number // 4), named(ordinary, number - number // 4 - 1))
    mixed = jax.random.permutation(jax.random.fold_in(own, 3), count)
    donor, taker = mixed[0:count // 2 * 2:2], mixed[1:count // 2 * 2:2]
    room = jnp.minimum(tallies[donor] - 1, reach - tallies[taker]) // 2
    room = jnp.where((donor == ranking[0]) | (taker == ranking[0]) | (tallies[taker] == 0), 0, jnp.maximum(room, 0))
    passed = jax.random.randint(jax.random.fold_in(own, 4), (count // 2,), 0, 1 << 20) % (room + 1)
    tallies = tallies.at[donor].add(-passed).at[taker].add(passed)
    members = jnp.searchsorted(jnp.cumsum(tallies), jnp.arange(rows * top), side="right").astype(jnp.int32)
    listing = members.reshape(top, rows).T
    listing = listing[jax.random.permutation(jax.random.fold_in(own, 1), rows)]
    turn = jax.random.randint(jax.random.fold_in(own, 2), (rows, 1), 0, top)
    return jnp.take_along_axis(listing, (jnp.arange(top)[None, :] + turn) % top, axis=1)


def load_shares(number_of, total, reach, skew, full):
    weights = [(1 << 20) // math.isqrt(rank ** skew) + 1 for rank in range(1, number_of + 1)]
    largest = reach if full else min(reach, max(-(-total // number_of), total * weights[0] // sum(weights)))
    least = 1 if total - largest >= number_of - 1 else 0
    given, rest = [largest] + [least] * (number_of - 1), total - largest - least * (number_of - 1)
    while rest > 0:
        movable = [i for i in range(1, number_of) if given[i] < largest] or [i for i in range(1, number_of) if given[i] < reach]
        whole, left = sum([weights[i] for i in movable]), rest
        for i in movable:
            addition = min(reach - given[i], max(1, left * weights[i] // whole), rest)
            given[i] = given[i] + addition
            rest = rest - addition
    return np.array(given)


def bell_draw(stream_key, dims, scale, reach, split=(), dtype=jnp.bfloat16):
    drawn = jax.random.normal(stream_key, dims, jnp.float32) * scale
    if len(split) > 0:
        drawn = block_scale(stream_key, dims, split, -0.22, 0.18) * drawn
    return jnp.clip(drawn, min=-reach, max=reach).astype(dtype)


def setup_inputs(seed: int = 0) -> dict:
    key_list = jax.random.split(jax.random.key(seed), 8)
    residual_stream = bell_draw(key_list[0], (TOKENS, D), 1.0, 6.0, ((0, 32),))
    norm_gain = jnp.clip(1.0 + 0.15 * jax.random.normal(key_list[1], (D,), jnp.float32), 0.25, 1.75)
    expert_ids_keys = jax.random.split(jax.random.fold_in(key_list[2], 1), TOKENS // TOK_DEV)
    expert_ids_turns = jax.random.permutation(jax.random.fold_in(key_list[2], 3), TOKENS // TOK_DEV)
    expert_ids = jax.vmap(lambda own, number: deal_out(jax.random.fold_in(key_list[2], 2), own, number, TOK_DEV, EXPERTS, TOP, CAP, 1))(expert_ids_keys, expert_ids_turns).reshape((TOKENS, TOP))
    gate_weights = jnp.clip(0.2 + 0.8 * jax.random.uniform(key_list[3], (TOKENS, TOP), jnp.float32) ** block_scale(key_list[3], (TOKENS, TOP), ((0, 32),), -0.2, 0.2), 0.2, 1.0)
    w_gate = bell_draw(key_list[4], (EXPERTS, D, FF), D ** -0.5, 0.09375, ((0, 8), (2, 4)))
    w_up = bell_draw(key_list[5], (EXPERTS, D, FF), D ** -0.5, 0.09375, ((0, 8), (2, 4)))
    w_down = bell_draw(key_list[6], (EXPERTS, FF, D), FF ** -0.5, 0.0625, ((0, 8), (1, 4)))
    return dict(residual_stream=residual_stream, norm_gain=norm_gain, expert_ids=expert_ids, gate_weights=gate_weights, w_gate=w_gate, w_up=w_up, w_down=w_down)


def one_expert(operands):
    rows, gate_w, up_w, down_w = operands
    gate = jnp.dot(rows, gate_w, preferred_element_type=jnp.float32)
    up = jnp.dot(rows, up_w, preferred_element_type=jnp.float32)
    hidden = (jax.nn.silu(gate) * up).astype(jnp.bfloat16)
    shard_width = FF // N_SEQ
    hidden_split = hidden.reshape(rows.shape[0], N_SEQ, shard_width).astype(jnp.float32)
    down_split = down_w.reshape(N_SEQ, shard_width, D).astype(jnp.float32)
    partial_value = jnp.einsum('rsf,sfd->srd', hidden_split, down_split).astype(jnp.bfloat16)
    return lax.optimization_barrier(jnp.sum(partial_value.astype(jnp.float32), axis=0))

def reference(residual_stream, norm_gain, expert_ids, gate_weights, w_gate, w_up, w_down):
    stream = residual_stream.astype(jnp.float32)
    power = lax.optimization_barrier(jnp.mean(stream * stream, axis=1, keepdims=True))
    features = (stream * lax.rsqrt(power + 1e-06) * norm_gain[None, :]).astype(jnp.bfloat16)
    blocks = TOKENS // TOK_DEV
    flat = expert_ids.reshape(blocks, TOP * TOK_DEV)
    labels = jnp.arange(EXPERTS).astype(jnp.int32)
    onehot = (flat[:, :, None] == labels[None, None, :]).astype(jnp.int32)
    before = jnp.cumsum(onehot, axis=1).astype(jnp.int32) - onehot
    slot = lax.optimization_barrier(jnp.sum(before * onehot, axis=2)).astype(jnp.int32)
    starts = (jnp.arange(blocks).astype(jnp.int32) * CAP)[:, None]
    position = (starts + slot).reshape(TOKENS, TOP).astype(jnp.int32)
    place = (expert_ids * (blocks * CAP) + position).astype(jnp.int32)
    repeated = jnp.repeat(features, TOP, axis=0)
    table = jnp.zeros((EXPERTS * blocks * CAP, D), jnp.bfloat16)
    table = table.at[place.reshape(-1)].set(repeated)
    table = table.reshape(EXPERTS, blocks * CAP, D)
    results = lax.map(one_expert, (table, w_gate, w_up, w_down))
    picked = results.reshape(EXPERTS * blocks * CAP, D)[place]
    combined = lax.optimization_barrier(jnp.sum(gate_weights[:, :, None] * picked, axis=1))
    return combined.astype(jnp.bfloat16)
```

```python
import functools
import jax
import jax.numpy as jnp
from jax import lax
from jax.experimental import pallas as pl
from jax.experimental.pallas import tpu as pltpu
from jax.sharding import PartitionSpec as P

F32 = jnp.float32
BF16 = jnp.bfloat16


def iota(shape, dim):
    return lax.broadcasted_iota(jnp.int32, shape, dim)


def routes_by_row(meta, me, core, main, count):
    tokens = meta.shape[1]
    shape = (count * main, tokens)
    expert = jnp.bitwise_xor(me, 2 * (iota(shape, 0) // main) + core).astype(F32)
    named = jnp.where((meta[0:1] == expert) | (meta[1:2] == expert), 1.0, 0.0)
    earlier = jnp.where(iota((tokens, tokens), 0) < iota((tokens, tokens), 1), 1.0, 0.0)
    rank = jnp.dot(named.astype(BF16), earlier.astype(BF16), preferred_element_type=F32)
    return jnp.where(named > 0, rank, -1.0)


def routes_by_token(meta, me, core, main, count):
    tokens = meta.shape[0]
    shape = (tokens, count * main)
    expert = jnp.bitwise_xor(me, 2 * (iota(shape, 1) // main) + core).astype(F32)
    first, second = meta[:, 0:1] == expert, meta[:, 1:2] == expert
    named = jnp.where(first | second, 1.0, 0.0)
    earlier = jnp.where(iota((tokens, tokens), 1) < iota((tokens, tokens), 0), 1.0, 0.0)
    rank = jnp.dot(earlier.astype(BF16), named.astype(BF16), preferred_element_type=F32)
    weight = jnp.where(first, meta[:, 2:3], jnp.where(second, meta[:, 3:4], 0.0))
    return jnp.where(named > 0, rank, -1.0), weight


def dispatch_kernel(count, main, extra, place, own, other, own_meta, other_meta, gain, *outs):
    me, core = place[0], place[1]
    width = own.shape[1]
    ext = extra * width // main
    for half, (stream_ref, meta) in enumerate(((own, own_meta), (other, other_meta))):
        stream = stream_ref[...].astype(F32)
        power = jnp.mean(stream * stream, axis=1, keepdims=True)
        features = (stream * lax.rsqrt(power + 1e-06) * gain[...]).astype(BF16)
        rank = routes_by_row(meta[...], me, core, main, count)
        line = iota(rank.shape, 0) % main
        pick = jnp.where(rank == line.astype(F32), 1.0, 0.0).astype(BF16)
        rows = jnp.dot(pick, features, preferred_element_type=F32).astype(BF16)
        past = rank == (main + line % extra).astype(F32)
        tail = None
        for piece in range(main // extra):
            pick = jnp.where(past & (line // extra == piece), 1.0, 0.0).astype(BF16)
            part = jnp.dot(
                pick, features[:, piece * ext : (piece + 1) * ext], preferred_element_type=F32
            )
            tail = part if tail is None else tail + part
        tail = tail.astype(BF16)
        for j in range(count):
            outs[j][half * main : (half + 1) * main, 0:width] = rows[j * main : (j + 1) * main]
            outs[j][half * main : (half + 1) * main, width:] = tail[j * main : (j + 1) * main]


def combine_kernel(count, main, extra, place, own_meta, other_meta, *refs):
    blocks, (own, other) = refs[:count], refs[count:]
    me, core = place[0], place[1]
    width = own.shape[1]
    ext = extra * width // main
    for half, (meta, out) in enumerate(((own_meta, own), (other_meta, other))):
        rank, weight = routes_by_token(meta[...], me, core, main, count)
        line = iota(rank.shape, 1) % main
        cut = [b[half * main : (half + 1) * main, :] for b in blocks]
        rows = jnp.concatenate([c[:, :width] for c in cut], axis=0)
        tail = jnp.concatenate([c[:, width:] for c in cut], axis=0)

        def product(weights, values):
            high = weights.astype(BF16)
            rest = weights - high.astype(F32)
            mid = rest.astype(BF16)
            low = (rest - mid.astype(F32)).astype(BF16)
            total = jnp.dot(high, values, preferred_element_type=F32)
            total += jnp.dot(mid, values, preferred_element_type=F32)
            return total + jnp.dot(low, values, preferred_element_type=F32)

        here = jnp.where(rank == line.astype(F32), weight, 0.0)
        past = rank == (main + line % extra).astype(F32)
        for piece in range(main // extra):
            span = slice(piece * ext, (piece + 1) * ext)
            late = jnp.where(past & (line // extra == piece), weight, 0.0)
            value = product(here, rows[:, span]) + product(late, tail)
            out[:, span] = value.astype(out.dtype)


def selector(shape, match):
    return jnp.where(match(iota(shape, 0), iota(shape, 1)), 1.0, 0.0).astype(BF16)


def ffn_kernel(count, groups, main, extra, ups, downs, *refs):
    blocks, (gate_w, up_w, down_w) = refs[:count], refs[count : count + 3]
    outs = refs[count + 3 : count + 3 + groups]
    table, ext_in, hidden, ext_out, sems = refs[count + 3 + groups :]
    step = pl.program_id(0)
    rows = ext_in.shape[0]
    height = rows // count
    past = table.shape[0] - rows
    width = table.shape[1]
    ext = ext_in.shape[1]
    wide = gate_w.shape[-1]
    per = rows // groups

    @pl.when(step == 0)
    def _():
        copies = []
        for q in range(count):
            spot = pl.ds(q * height, height)
            copies.append(
                pltpu.make_async_copy(
                    blocks[q].at[:, pl.ds(0, width)], table.at[spot, :], sems.at[0, q]
                )
            )
            copies.append(
                pltpu.make_async_copy(
                    blocks[q].at[:, pl.ds(width, ext)], ext_in.at[spot, :], sems.at[1, q]
                )
            )
        for c in copies:
            c.start()
        for c in copies:
            c.wait()
        for piece in range(width // ext):
            pick = selector(
                (past, rows),
                lambda r, c: c == (r // extra) * main + extra * piece + r % extra,
            )
            table[pl.ds(rows, past), pl.ds(piece * ext, ext)] = jnp.dot(
                pick, ext_in[...], preferred_element_type=F32
            ).astype(BF16)
        ext_out[...] = jnp.zeros_like(ext_out)

    @pl.when(step < ups)
    def _():
        x = table[...]
        gate = jnp.dot(x, gate_w[...], preferred_element_type=F32)
        up = jnp.dot(x, up_w[...], preferred_element_type=F32)
        value = (gate / (1.0 + jnp.exp(-gate)) * up).astype(BF16)
        hidden[:, pl.ds(pl.multiple_of(step * wide, wide), wide)] = value

    @pl.when((step >= ups) & (step < ups + downs))
    def _():
        piece = step - ups
        partial = jnp.dot(hidden[...], down_w[...], preferred_element_type=F32).astype(BF16)
        for q in range(groups):
            outs[q][...] = partial[q * per : (q + 1) * per]
        pick = selector(
            (rows, past), lambda r, c: r == (c // extra) * main + extra * piece + c % extra
        )
        ext_out[...] += jnp.dot(pick, partial[rows:], preferred_element_type=F32)

    @pl.when(step == ups + downs)
    def _():
        value = ext_out[...].astype(BF16)
        for q in range(groups):
            outs[q][...] = value[q * per : (q + 1) * per]


def ffn(blocks, gate_w, up_w, down_w, main, extra, groups, wide=256):
    count, height = len(blocks), blocks[0].shape[0]
    width, ff = gate_w.shape
    ext = extra * width // main
    rows = count * height
    past = rows // main * extra
    ups, downs = ff // wide, width // ext
    up_spec = pl.BlockSpec((width, wide), lambda i: (0, jnp.minimum(i, ups - 1)))
    return pl.pallas_call(
        functools.partial(ffn_kernel, count, groups, main, extra, ups, downs),
        grid=(ups + downs + 1,),
        in_specs=[pl.BlockSpec(memory_space=pltpu.HBM)] * count
        + [
            up_spec,
            up_spec,
            pl.BlockSpec((ff, ext), lambda i: (0, jnp.clip(i - ups, 0, downs - 1))),
        ],
        out_specs=[
            pl.BlockSpec((rows // groups, ext), lambda i: (0, jnp.clip(i - ups, 0, downs)))
        ]
        * groups,
        out_shape=[jax.ShapeDtypeStruct((rows // groups, width + ext), BF16)] * groups,
        scratch_shapes=[
            pltpu.VMEM((rows + past, width), BF16),
            pltpu.VMEM((rows, ext), BF16),
            pltpu.VMEM((rows + past, ff), BF16),
            pltpu.VMEM((rows, ext), F32),
            pltpu.SemaphoreType.DMA((2, count)),
        ],
        cost_estimate=pl.CostEstimate(
            flops=6 * (rows + past) * width * ff,
            bytes_accessed=6 * width * ff + 4 * rows * (width + ext),
            transcendentals=(rows + past) * ff,
        ),
        compiler_params=pltpu.CompilerParams(vmem_limit_bytes=60 * 1024 * 1024),
        name="ffn",
    )(*blocks, gate_w, up_w, down_w)


def per_device(residual_stream, norm_gain, expert_ids, gate_weights, w_gate, w_up, w_down):
    tokens, width = residual_stream.shape
    top = expert_ids.shape[1]
    n_exp, n_seq = lax.axis_size("exp"), lax.axis_size("seq")
    experts = n_exp * w_gate.shape[0]
    main, extra = top * tokens // experts, 2
    ext = extra * width // main
    pairs, sides = n_exp // 2, n_seq // 2
    me, core = lax.axis_index("exp"), lax.axis_index("seq") % 2
    place = jnp.stack([me, core]).astype(jnp.int32)

    def over_seq(value, flip):
        return lax.ppermute(value, "seq", [(s, s ^ flip) for s in range(n_seq)])

    def over_exp(value, j):
        return lax.ppermute(
            value,
            ("seq", "exp"),
            [
                (s * n_exp + e, s * n_exp + (e ^ (2 * j + s % 2)))
                for s in range(n_seq)
                for e in range(n_exp)
            ],
        )

    meta = jnp.concatenate([expert_ids.astype(F32), gate_weights], axis=1)
    other = over_seq(residual_stream, 1)
    other_meta = over_seq(meta, 1)

    vmem = pl.BlockSpec(memory_space=pltpu.VMEM)
    smem = pl.BlockSpec(memory_space=pltpu.SMEM)
    blocks = pl.pallas_call(
        functools.partial(dispatch_kernel, pairs, main, extra),
        in_specs=[smem] + [vmem] * 5,
        out_specs=[vmem] * pairs,
        out_shape=[jax.ShapeDtypeStruct((2 * main, width + ext), BF16)] * pairs,
        compiler_params=pltpu.CompilerParams(vmem_limit_bytes=40 << 20),
        name="dispatch",
    )(place, residual_stream, other, meta.T, other_meta.T, norm_gain[None, :])

    order = list(range(pairs - 1, -1, -1))
    came = {j: over_exp(blocks[j], j) for j in order}
    held = []
    near, far = {}, {}
    for j in range(pairs):
        near[j] = [came[j]] + [over_seq(came[j], 2 * m) for m in range(1, sides)]
        far[j] = [over_seq(v, 1) for v in near[j]]
    for group in (near, far):
        for j in range(pairs):
            held += group[j]
    outs = ffn(held, w_gate[0], w_up[0], w_down[0], main, extra, 2 * pairs)

    height = 2 * main
    final = {}
    for j in order:
        kept, sent = outs[j], outs[pairs + j]
        total = kept.astype(F32) + over_seq(sent, 1).astype(F32)
        own = total[:height]
        for m in range(1, sides):
            own = own + over_seq(
                total[m * height : (m + 1) * height].astype(BF16), 2 * m
            ).astype(F32)
        final[j] = over_exp(own.astype(BF16), j)

    mine, theirs = pl.pallas_call(
        functools.partial(combine_kernel, pairs, main, extra),
        in_specs=[smem] + [vmem] * (2 + pairs),
        out_specs=[vmem] * 2,
        out_shape=[
            jax.ShapeDtypeStruct((tokens, width), F32),
            jax.ShapeDtypeStruct((tokens, width), BF16),
        ],
        compiler_params=pltpu.CompilerParams(vmem_limit_bytes=40 << 20),
        name="combine",
    )(place, meta, other_meta, *[final[j] for j in range(pairs)])
    return (mine + over_seq(theirs, 1).astype(F32)).astype(BF16)


def solution(mesh):
    in_specs = (
        P(("seq", "exp"), None),
        P(),
        P(("seq", "exp"), None),
        P(("seq", "exp"), None),
        P("exp", None, "seq"),
        P("exp", None, "seq"),
        P("exp", "seq", None),
    )
    out_specs = P(("seq", "exp"), None)
    return jax.shard_map(
        per_device, mesh=mesh, in_specs=in_specs, out_specs=out_specs, check_vma=False
    )
```
